256 devices in a mesh: trial: 4 (over z_lo), lat: 2 (over z_hi), lon: 4 (over x_hi, core), lev: 8 (over y, x_lo).
Axes of the slice: x: 4 (x_hi: 2, x_lo: 2; x = x_hi * 2 + x_lo), y: 4, z: 8 (z_hi: 2, z_lo: 4; z = z_hi * 4 + z_lo), core: 2. Of those that a mesh axis runs over, the one named last changes fastest.
Arguments:
- density: float32 [32, 64, 1024, 128], P(('trial', 'lat'), 'lon', 'lev'), parts along dimension 0, may hold values from 0.5 to 2
- crowding: float32 [32, 64, 1024, 128], P(('trial', 'lat'), 'lon', 'lev'), parts along dimension 0, may hold values from 0.5 to 2
Outputs:
- scaled_field: float32 [32, 64, 1024, 128], P(('trial', 'lat'), 'lon', 'lev'), parts along dimension 0
- density_end: float32 [32, 64, 1024, 128], P(('trial', 'lat'), 'lon', 'lev'), parts along dimension 0
The draws below stay inside these ranges and needn't reach their ends.
There are 4 independent parts, one for each index of `trial`. The reference program is written for one: setup_inputs(seed, part) draws one part's arguments, and reference() takes and returns one part's arrays. A program takes and returns all parts, laid end to end along the dimension named above; each array names one. Nothing has to cross between parts.
All inputs are finite; a program needn't handle non-finite values.
Results may differ from the reference program's by a relative error of at most 0.000058.
Values sent between devices are 32-bit elements; how exact they have to be, the bound alone decides.
No kernel may reach another device: no remote copies, remote signals or barrier semaphores. Data moves between devices by JAX's collectives and lax.ppermute only.
A program may use at most 64 MiB of HBM per device.

```python
import jax
import jax.numpy as jnp
from jax import lax

GRID_Y = 8
GRID_X = 64
GRID_Z = 1024
SPECIES = 128
STEPS = 4


def shard_levels(stream_key, extent, cuts, least, largest):
    level, own = 1.0, jax.random.fold_in(stream_key, 6)
    for dim, blocks in cuts:
        draws = jnp.exp(jax.random.uniform(jax.random.fold_in(own, dim), (blocks,), jnp.float32, least / len(cuts), largest / len(cuts)))
        level = level * jnp.repeat(draws, extent[dim] // blocks).reshape([-1 if axis == dim else 1 for axis in range(len(extent))])
    return level


def setup_inputs(seed: int = 0, part: int = 0) -> dict:
    arg_keys = jax.random.split(jax.random.key(seed), 3)
    own_keys = jax.random.split(jax.random.fold_in(arg_keys[2], part), 3)
    density = jnp.clip(0.5 + 1.5 * jax.random.uniform(own_keys[0], (GRID_Y, GRID_X, GRID_Z, SPECIES), jnp.float32) ** shard_levels(own_keys[0], (GRID_Y, GRID_X, GRID_Z, SPECIES), ((0, 2), (1, 4), (2, 8)), -0.2, 0.2), 0.5, 2.0)
    crowding = jnp.clip(0.5 + 1.5 * jax.random.uniform(own_keys[1], (GRID_Y, GRID_X, GRID_Z, SPECIES), jnp.float32) ** shard_levels(own_keys[1], (GRID_Y, GRID_X, GRID_Z, SPECIES), ((0, 2), (1, 4), (2, 8)), -0.2, 0.2), 0.5, 2.0)
    return dict(density=density, crowding=crowding)


def inner_cells(values, dims):
    for dim in dims:
        values = lax.slice_in_dim(values, 1, values.shape[dim] - 1, axis=dim)
    return values

def side_cells(values, dim, start, dims):
    others = [other for other in dims if other != dim]
    values = inner_cells(values, others)
    return lax.slice_in_dim(values, start, start + values.shape[dim] - 2, axis=dim)

def advance(padded, crowding):
    middle = inner_cells(padded, (0, 1, 2))
    lower = [side_cells(padded, dim, 0, (0, 1, 2)) for dim in (0, 1, 2)]
    upper = [side_cells(padded, dim, 2, (0, 1, 2)) for dim in (0, 1, 2)]
    spread = lower[0] + upper[0] + lower[1] + upper[1] + lower[2] + upper[2] - 6.0 * middle
    return middle + 0.1 * spread + 0.2 * middle * (1.0 - middle * crowding)

def reference(density, crowding):
    for step in range(STEPS):
        density = advance(jnp.pad(density, ((1, 1), (1, 1), (1, 1), (0, 0)), mode='constant'), crowding)
    line_mean = lax.optimization_barrier(jnp.mean(density, axis=1, keepdims=True))
    centred = density - line_mean
    line_variance = lax.optimization_barrier(jnp.mean(centred * centred, axis=1, keepdims=True))
    scaled_field = centred * lax.rsqrt(line_variance + 0.0001)
    return (scaled_field, density)
```

```python
import functools

import jax
import jax.numpy as jnp
from jax import lax
from jax.experimental import pallas as pl
from jax.experimental.pallas import tpu as pltpu
from jax.sharding import PartitionSpec as P

STEPS = 4
MIB = 1 << 20


def cells(a, low_x, high_x, near, far, low_z, high_z, crowding):
    length = a.shape[0]
    z = lax.broadcasted_iota(jnp.int32, a.shape, 0)
    down = jnp.where(z == 0, low_z, pltpu.roll(a, 1, 0))
    up = jnp.where(z == length - 1, high_z, pltpu.roll(a, length - 1, 0))
    spread = low_x + high_x + near + far + down + up - 6.0 * a
    return a + 0.1 * spread + 0.2 * a * (1.0 - a * crowding)


def over_x(n, visit):
    visit(0, None, 1)

    def inner(x, carry):
        visit(x, x - 1, x + 1)
        return carry

    lax.fori_loop(1, n - 1, inner, 0)
    visit(n - 1, n - 2, None)


def line_sums(column, n, mean_store, m2_store):
    total = lax.fori_loop(1, n, lambda x, s: s + column(x), column(0))
    mean = total / n
    mean_store(mean)

    def add(x, s):
        d = column(x) - mean
        return s + d * d

    m2_store(lax.fori_loop(0, n, add, jnp.zeros_like(mean)))


def row_kernel(first, last, stats, *refs):
    centre, near, far, crowding, x_low, x_high, z_low, z_high, out = refs[:9]
    n = centre.shape[0]

    def visit(x, before, after):
        low_x = x_low[0] if before is None else centre[before]
        high_x = x_high[0] if after is None else centre[after]
        low_z = z_low[0, pl.ds(x, 1), :] if first else z_low[x, 7:8, :]
        high_z = z_high[0, pl.ds(x, 1), :] if last else z_high[x, 0:1, :]
        out[x] = cells(centre[x], low_x, high_x, near[x], far[0, x], low_z, high_z, crowding[x])

    over_x(n, visit)
    if stats:
        sums = refs[9]

        def put(k, value):
            sums[k] = value

        line_sums(lambda x: out[x], n, functools.partial(put, 0), functools.partial(put, 1))


def row_step(c, chunks, received, rest, crowding, ghosts, stats):
    x_low, x_high, z_low, z_high = ghosts
    centre = chunks[c]
    n, depth, species = centre.shape
    count = len(chunks)
    first, last = c == 0, c == count - 1
    whole = pl.BlockSpec(memory_space=pltpu.VMEM)
    chunk = lambda: pl.BlockSpec((1, depth, species), lambda i: (0, c, 0))
    edge = lambda at: pl.BlockSpec((n, 8, species), lambda i: (0, at, 0))
    ghost = lambda: pl.BlockSpec((1, n, species), lambda i: (0, 0, 0))
    full = lambda: pl.BlockSpec((n, depth, species), lambda i: (0, 0, 0))
    out_shape = [jax.ShapeDtypeStruct(centre.shape, jnp.float32)]
    out_specs = [full()]
    if stats:
        out_shape.append(jax.ShapeDtypeStruct((2, depth, species), jnp.float32))
        out_specs.append(pl.BlockSpec((2, depth, species), lambda i: (0, 0, 0)))
    result = pl.pallas_call(
        functools.partial(row_kernel, first, last, stats),
        grid=(1,),
        out_shape=out_shape,
        in_specs=[
            full(),
            full(),
            pl.BlockSpec((1, n, depth, species), lambda i: (0, 0, c, 0)),
            full(),
            chunk(),
            chunk(),
            ghost() if first else edge(chunks[c - 1].shape[1] // 8 - 1),
            ghost() if last else edge(0),
        ],
        out_specs=out_specs,
        compiler_params=pltpu.CompilerParams(vmem_limit_bytes=16 * MIB),
        cost_estimate=pl.CostEstimate(
            flops=20 * centre.size, bytes_accessed=20 * centre.size, transcendentals=0
        ),
        name=f"row_chunk_{c}",
    )(
        centre,
        received,
        rest,
        crowding,
        x_low,
        x_high,
        z_low if first else chunks[c - 1],
        z_high if last else chunks[c + 1],
    )
    return result if stats else (result[0], None)


def rest_kernel(count, mapped, stats, *refs):
    order = refs[0]
    chunks, refs = refs[1 : 1 + count], refs[1 + count :]
    field, crowding, x_low, x_high, z_low, z_high, out = refs[:7]
    n, length = field.shape[1], field.shape[2]

    for row in range(3):
        at = order[row + 1] if mapped else row
        beyond = None if row == 2 else (order[row + 2] if mapped else row + 1)
        before_row = None if row == 0 else (order[row] if mapped else row - 1)
        crowd_at = order[row + 1]

        def visit(x, before, after):
            low_x = x_low[row + 1] if before is None else field[at, before]
            high_x = x_high[row + 1] if after is None else field[at, after]
            if row == 0:
                near = jnp.concatenate([part[x] for part in chunks], axis=0)
            else:
                near = field[before_row, x]
            far = 0.0 if beyond is None else field[beyond, x]
            low_z = z_low[row + 1, pl.ds(x, 1), :]
            high_z = z_high[row + 1, pl.ds(x, 1), :]
            out[row, x] = cells(
                field[at, x], low_x, high_x, near, far, low_z, high_z, crowding[crowd_at, x]
            )

        over_x(n, visit)
        if stats:
            sums = refs[7]

            def put(k, value):
                sums[k, row] = value

            line_sums(lambda x: out[row, x], n, functools.partial(put, 0), functools.partial(put, 1))


def rest_step(order, chunks, field, crowding, ghosts, mapped, stats):
    _, n, length, species = field.shape
    vmem = pl.BlockSpec(memory_space=pltpu.VMEM)
    out_shape = [jax.ShapeDtypeStruct((3, n, length, species), jnp.float32)]
    if stats:
        out_shape.append(jax.ShapeDtypeStruct((2, 3, length, species), jnp.float32))
    size = 3 * n * length * species
    result = pl.pallas_call(
        functools.partial(rest_kernel, len(chunks), mapped, stats),
        out_shape=out_shape,
        in_specs=[pl.BlockSpec(memory_space=pltpu.SMEM)] + [vmem] * (len(chunks) + 6),
        out_specs=[vmem] * len(out_shape),
        compiler_params=pltpu.CompilerParams(vmem_limit_bytes=24 * MIB),
        cost_estimate=pl.CostEstimate(
            flops=20 * size, bytes_accessed=16 * size, transcendentals=0
        ),
        name="rest",
    )(order, *chunks, field, crowding, *ghosts)
    return result if stats else (result[0], None)


def whole_lines(parts, n):
    mean = (parts[0][0] + parts[1][0] + parts[2][0] + parts[3][0]) / 4
    m2 = parts[0][1] + parts[1][1] + parts[2][1] + parts[3][1]
    between = jnp.zeros_like(mean)
    for part in parts:
        d = part[0] - mean
        between = between + d * d
    variance = (m2 + n * between) / (4 * n)
    return mean, lax.rsqrt(variance + 0.0001)


def place_kernel(order, field, s0, s1, s2, s3, scaled, density):
    n = field.shape[1]
    for row in range(3):
        at = order[row + 1]
        mean, factor = whole_lines([[s[0, row], s[1, row]] for s in (s0, s1, s2, s3)], n)

        def visit(x, carry):
            value = field[row, x]
            density[at, x] = value
            scaled[at, x] = (value - mean) * factor
            return carry

        lax.fori_loop(0, n, visit, 0)


def place_rest(order, field, parts):
    _, n, length, species = field.shape
    vmem = pl.BlockSpec(memory_space=pltpu.VMEM)
    whole = jax.ShapeDtypeStruct((4, n, length, species), jnp.float32)
    size = 3 * n * length * species
    return pl.pallas_call(
        place_kernel,
        out_shape=[whole, whole],
        in_specs=[pl.BlockSpec(memory_space=pltpu.SMEM)] + [vmem] * 5,
        out_specs=[vmem, vmem],
        compiler_params=pltpu.CompilerParams(vmem_limit_bytes=24 * MIB),
        cost_estimate=pl.CostEstimate(
            flops=10 * size, bytes_accessed=16 * size, transcendentals=0
        ),
        name="place_rest",
    )(order, field, *parts)


def place_row_kernel(order, field, s0, s1, s2, s3, scaled_in, density_in, scaled, density):
    n = field.shape[0]
    mean, factor = whole_lines([[s[0], s[1]] for s in (s0, s1, s2, s3)], n)

    def visit(x, carry):
        value = field[x]
        density[0, x] = value
        scaled[0, x] = (value - mean) * factor
        return carry

    lax.fori_loop(0, n, visit, 0)


def place_row(order, at, field, parts, scaled, density):
    n, depth, species = field.shape
    block = at // depth
    out = lambda: pl.BlockSpec((1, n, depth, species), lambda i, order: (order[0], 0, block, 0))
    return pl.pallas_call(
        place_row_kernel,
        grid_spec=pltpu.PrefetchScalarGridSpec(
            num_scalar_prefetch=1,
            grid=(1,),
            in_specs=[pl.BlockSpec((n, depth, species), lambda i, order: (0, 0, 0))]
            + [pl.BlockSpec((2, depth, species), lambda i, order: (0, 0, 0))] * 4
            + [pl.BlockSpec(memory_space=pl.ANY)] * 2,
            out_specs=[out(), out()],
        ),
        out_shape=[jax.ShapeDtypeStruct(scaled.shape, jnp.float32)] * 2,
        input_output_aliases={6: 0, 7: 1},
        compiler_params=pltpu.CompilerParams(vmem_limit_bytes=16 * MIB),
        cost_estimate=pl.CostEstimate(
            flops=10 * field.size, bytes_accessed=12 * field.size, transcendentals=0
        ),
        name="place_row",
    )(order, field, *parts, scaled, density)


def both_ways(low, high, axis):
    devices = lax.axis_size(axis)
    up = [(i, i + 1) for i in range(devices - 1)]
    return lax.ppermute(high, axis, up), lax.ppermute(low, axis, [(b, a) for a, b in up])


def everyones(array, axis):
    devices = lax.axis_size(axis)
    shifted = [
        lax.ppermute(array, axis, [(i, (i + k) % devices) for i in range(devices)])
        for k in range(1, devices)
    ]
    return [array, *shifted]


def shards(density, crowding):
    lat = lax.axis_index("lat")
    rows, n, length, species = density.shape
    cuts = (0, length // 2, length)
    order = jnp.where(lat == 0, jnp.arange(rows)[::-1], jnp.arange(rows)).astype(jnp.int32)

    def logical(edges):
        return jnp.where(lat == 0, edges[::-1], edges)

    def pieces(array):
        row = lax.dynamic_index_in_dim(array, order[0], 0, keepdims=False)
        return [row[:, a:b] for a, b in zip(cuts[:-1], cuts[1:])]

    swap = [(0, 1), (1, 0)]
    chunks = pieces(density)
    arriving = [lax.ppermute(c, "lat", swap) for c in chunks]
    x_edges = (logical(density[:, 0]), logical(density[:, n - 1]))
    z_edges = (logical(density[:, :, 0]), logical(density[:, :, length - 1]))
    crowd = pieces(crowding)
    rest = lax.dynamic_index_in_dim(density, order[1], 0)
    for step in range(STEPS):
        ghosts = (*both_ways(*x_edges, "lon"), *both_ways(*z_edges, "lev"))
        final = step == STEPS - 1
        new, sums = [], []
        rest_new, rest_sums = rest_step(
            order, chunks, density if step == 0 else rest, crowding, ghosts, step == 0, final
        )
        sent = []
        for c in range(len(chunks)):
            value, s = row_step(c, chunks, arriving[c], rest, crowd[c], ghosts, final)
            new.append(value)
            sums.append(s)
            if not final:
                sent.append(lax.ppermute(value, "lat", swap))
        chunks, rest, arriving = new, rest_new, sent
        if not final:
            row_x = [jnp.concatenate([c[at] for c in chunks], axis=0)[None] for at in (0, n - 1)]
            x_edges = [
                jnp.concatenate([row_x[k], rest[:, at]], axis=0) for k, at in enumerate((0, n - 1))
            ]
            z_edges = (
                jnp.concatenate([chunks[0][None, :, 0], rest[:, :, 0]], axis=0),
                jnp.concatenate([chunks[-1][None, :, -1], rest[:, :, length - 1]], axis=0),
            )
    scaled, ended = place_rest(order, rest, everyones(rest_sums, "lon"))
    for c, value in enumerate(chunks):
        scaled, ended = place_row(order, cuts[c], value, everyones(sums[c], "lon"), scaled, ended)
    return scaled, ended


def solution(mesh):
    placed = P(("trial", "lat"), "lon", "lev", None)
    return jax.shard_map(
        shards,
        mesh=mesh,
        in_specs=(placed, placed),
        out_specs=(placed, placed),
        check_vma=False,
    )
```

```python
import functools

import jax
import jax.numpy as jnp
from jax import lax
from jax.experimental import pallas as pl
from jax.experimental.pallas import tpu as pltpu
from jax.sharding import PartitionSpec as P


STEPS = 4
MIB = 1 << 20
EVEN_X, EVEN_Z = 4, 5
VMEM = pl.BlockSpec(memory_space=pltpu.VMEM)
SMEM = pl.BlockSpec(memory_space=pltpu.SMEM)
ANY = pl.BlockSpec(memory_space=pl.ANY)


def cost(size, flops, reads):
    return pl.CostEstimate(flops=flops * size, bytes_accessed=4 * reads * size, transcendentals=0)


def cells(a, low_x, high_x, near, far, low_z, high_z, crowding):
    length = a.shape[0]
    z = lax.broadcasted_iota(jnp.int32, a.shape, 0)
    down = jnp.where(z == 0, low_z, pltpu.roll(a, 1, 0))
    up = jnp.where(z == length - 1, high_z, pltpu.roll(a, length - 1, 0))
    spread = low_x + high_x + near + far + down + up - 6.0 * a
    return a + 0.1 * spread + 0.2 * a * (1.0 - a * crowding)


def over_x(n, visit):
    visit(0, None, 1)

    def inner(x, carry):
        visit(x, x - 1, x + 1)
        return carry

    lax.fori_loop(1, n - 1, inner, 0)
    visit(n - 1, n - 2, None)


def line_sums(column, n):
    mean = lax.fori_loop(1, n, lambda x, s: s + column(x), column(0)) / n

    def add(x, s):
        d = column(x) - mean
        return s + d * d

    return mean, lax.fori_loop(0, n, add, jnp.zeros_like(mean))


def sides(info, row, ghosts):
    lon_a, lon_b, lev_a, lev_b = ghosts
    even_x, even_z = info[EVEN_X] == 1, info[EVEN_Z] == 1
    low_x = lambda: jnp.where(even_x, lon_b[row], lon_a[row])
    high_x = lambda: jnp.where(even_x, lon_a[row], lon_b[row])

    def ends_z(x):
        a, b = lev_a[row, pl.ds(x, 1), :], lev_b[row, pl.ds(x, 1), :]
        return jnp.where(even_z, b, a), jnp.where(even_z, a, b)

    return low_x, high_x, ends_z


def edge_kernel(mapped, info, *refs):
    if mapped:
        field, lon_a, lon_b, lev_a, lev_b = refs
        rows = [field.at[info[row]] for row in range(4)]
    else:
        first, field, lon_a, lon_b, lev_a, lev_b = refs
        rows = [first, *(field.at[row] for row in range(3))]
    n, length = rows[0].shape[0], rows[0].shape[1]
    for row, values in enumerate(rows):
        at = info[EVEN_X] * (n - 1)
        lon_a[row] = values[at]
        lon_b[row] = values[n - 1 - at]
        at = info[EVEN_Z] * (length - 1)
        for x in range(n):
            lev_a[row, x : x + 1, :] = values[x, pl.ds(at, 1), :]
            lev_b[row, x : x + 1, :] = values[x, pl.ds(length - 1 - at, 1), :]


def edges(info, first, field):
    mapped = first is None
    _, n, length, species = field.shape
    lon = jax.ShapeDtypeStruct((4, length, species), jnp.float32)
    lev = jax.ShapeDtypeStruct((4, n, species), jnp.float32)
    args = [field] if mapped else [first, field]
    return pl.pallas_call(
        functools.partial(edge_kernel, mapped),
        out_shape=[lon, lon, lev, lev],
        in_specs=[SMEM] + [VMEM] * len(args),
        out_specs=[VMEM] * 4,
        compiler_params=pltpu.CompilerParams(vmem_limit_bytes=16 * MIB),
        cost_estimate=cost(8 * (length + n) * species, 1, 2),
        name="edges",
    )(info, *args)


def row_kernel(info, centre, near, far, crowding, lon_a, lon_b, lev_a, lev_b, *out):
    new = out[0]
    n = centre.shape[0]
    low, high, ends_z = sides(info, 0, (lon_a, lon_b, lev_a, lev_b))

    def visit(x, before, after):
        low_x = low() if before is None else centre[before]
        high_x = high() if after is None else centre[after]
        low_z, high_z = ends_z(x)
        new[x] = cells(
            centre[x], low_x, high_x, near[x], far[0, x], low_z, high_z, crowding[0, x]
        )

    over_x(n, visit)


def row_end_kernel(info, centre, near, far, crowding, lon_a, lon_b, lev_a, lev_b, _, new, sums, ended, sem):
    row_kernel(info, centre, near, far, crowding, lon_a, lon_b, lev_a, lev_b, new)
    copy = pltpu.make_async_copy(new, ended.at[info[0]], sem)
    copy.start()
    sums[0], sums[1] = line_sums(lambda x: new[x], centre.shape[0])
    copy.wait()


def row_step(info, centre, received, field, crowding, ghosts, mapped, ended=None):
    n, length, species = centre.shape
    full = lambda a: pl.BlockSpec(a.shape, lambda i, info: (0,) * a.ndim)
    one = (1, n, length, species)
    out_shape = [jax.ShapeDtypeStruct(centre.shape, jnp.float32)]
    out_specs = [full(centre)]
    extra, more = [], {}
    if ended is not None:
        out_shape += [
            jax.ShapeDtypeStruct((2, length, species), jnp.float32),
            jax.ShapeDtypeStruct(ended.shape, jnp.float32),
        ]
        out_specs += [full(out_shape[1]), ANY]
        extra, more = [ended], {"input_output_aliases": {9: 2}}
    return pl.pallas_call(
        row_kernel if ended is None else row_end_kernel,
        grid_spec=pltpu.PrefetchScalarGridSpec(
            num_scalar_prefetch=1,
            grid=(1,),
            in_specs=[
                full(centre),
                full(received),
                pl.BlockSpec(one, lambda i, info: (info[1] if mapped else 0, 0, 0, 0)),
                pl.BlockSpec(one, lambda i, info: (info[0], 0, 0, 0)),
                *map(full, ghosts),
                *([ANY] * len(extra)),
            ],
            out_specs=out_specs,
            scratch_shapes=[pltpu.SemaphoreType.DMA] * len(extra),
        ),
        out_shape=out_shape,
        compiler_params=pltpu.CompilerParams(vmem_limit_bytes=20 * MIB),
        cost_estimate=cost(centre.size, 20, 5),
        name="row",
        **more,
    )(info, centre, received, field, crowding, *ghosts, *extra)


def rest_kernel(mapped, final, info, *refs):
    if mapped:
        first, refs = None, refs
    else:
        first, refs = refs[0], refs[1:]
    field, crowding, lon_a, lon_b, lev_a, lev_b, out = refs[:7]
    n = field.shape[1]
    copies = []
    for row in range(3):
        at = info[row + 1] if mapped else row
        beyond = info[row + 2] if mapped and row < 2 else row + 1
        crowd_at = info[row + 1]
        low, high, ends_z = sides(info, row + 1, (lon_a, lon_b, lev_a, lev_b))

        def visit(x, before, after):
            low_x = low() if before is None else field[at, before]
            high_x = high() if after is None else field[at, after]
            if mapped:
                near = field[info[row], x]
            else:
                near = first[x] if row == 0 else field[row - 1, x]
            far = 0.0 if row == 2 else field[beyond, x]
            low_z, high_z = ends_z(x)
            out[row, x] = cells(
                field[at, x], low_x, high_x, near, far, low_z, high_z, crowding[crowd_at, x]
            )

        over_x(n, visit)
        if final:
            sums, ended, sem = refs[7:]
            copies.append(pltpu.make_async_copy(out.at[row], ended.at[info[row + 1]], sem.at[row]))
            copies[-1].start()
            sums[0, row], sums[1, row] = line_sums(lambda x: out[row, x], n)
    for copy in copies:
        copy.wait()


def rest_step(info, first, field, crowding, ghosts, final):
    mapped = first is None
    _, n, length, species = field.shape
    out_shape = [jax.ShapeDtypeStruct((3, n, length, species), jnp.float32)]
    out_specs, scratch = [VMEM], []
    if final:
        out_shape += [
            jax.ShapeDtypeStruct((2, 3, length, species), jnp.float32),
            jax.ShapeDtypeStruct((4, n, length, species), jnp.float32),
        ]
        out_specs += [VMEM, ANY]
        scratch = [pltpu.SemaphoreType.DMA((3,))]
    args = [*([] if mapped else [first]), field, crowding, *ghosts]
    return pl.pallas_call(
        functools.partial(rest_kernel, mapped, final),
        out_shape=out_shape,
        in_specs=[SMEM] + [VMEM] * len(args),
        out_specs=out_specs,
        scratch_shapes=scratch,
        compiler_params=pltpu.CompilerParams(vmem_limit_bytes=24 * MIB),
        cost_estimate=cost(3 * n * length * species, 20, 4),
        name="rest",
    )(info, *args)


def merged(a, b, n):
    d = a[0] - b[0]
    return jnp.stack([0.5 * (a[0] + b[0]), a[1] + b[1] + (0.5 * n) * d * d])


def line_factors(a, b, n):
    d = a[0] - b[0]
    variance = (a[1] + b[1] + (0.5 * n) * d * d) / (2 * n)
    return 0.5 * (a[0] + b[0]), lax.rsqrt(variance + 0.0001)


def scale_kernel(rows, info, field, one, two, *refs):
    scaled, buffer, sem = refs[-3:]
    n = buffer.shape[1]
    copies = []
    for k, row in enumerate(rows):
        values = field if len(rows) == 1 else field.at[k]
        mean, factor = line_factors(*([s[0, k], s[1, k]] for s in (one, two)), 2 * n)

        def visit(x, carry):
            buffer[k, x] = (values[x] - mean) * factor
            return carry

        lax.fori_loop(0, n, visit, 0)
        copies.append(pltpu.make_async_copy(buffer.at[k], scaled.at[info[row]], sem.at[k]))
        copies[-1].start()
    for copy in copies:
        copy.wait()


def scale(info, rows, field, one, two, scaled=None):
    n, length, species = field.shape[-3:]
    count = len(rows)
    whole = jax.ShapeDtypeStruct((4, n, length, species), jnp.float32)
    extra, more = ([], {}) if scaled is None else ([scaled], {"input_output_aliases": {4: 0}})
    return pl.pallas_call(
        functools.partial(scale_kernel, rows),
        out_shape=whole,
        in_specs=[SMEM] + [VMEM] * 3 + [ANY] * len(extra),
        out_specs=ANY,
        scratch_shapes=[
            pltpu.VMEM((count, n, length, species), jnp.float32),
            pltpu.SemaphoreType.DMA((count,)),
        ],
        compiler_params=pltpu.CompilerParams(vmem_limit_bytes=16 * MIB),
        cost_estimate=cost(field.size, 3, 2),
        name="scale",
        **more,
    )(info, field, one, two, *extra)


def paired(array, axis, pairs):
    return lax.ppermute(array, axis, [*pairs, *((b, a) for a, b in pairs)])


def exchanged(sent):
    lon_a, lon_b, lev_a, lev_b = sent
    return (
        paired(lon_a, "lon", [(0, 1), (2, 3)]),
        paired(lon_b, "lon", [(1, 2)]),
        paired(lev_a, "lev", [(0, 1), (2, 3), (4, 5), (6, 7)]),
        paired(lev_b, "lev", [(1, 2), (3, 4), (5, 6)]),
    )


def halves_of_lines(sums, n):
    half = merged(sums, paired(sums, "lon", [(0, 1), (2, 3)]), n)
    return half, paired(half, "lon", [(0, 2), (1, 3)])


def steps(density, crowding):
    rows, n, _, _ = density.shape
    flipped = lax.axis_index("lat") == 0
    order = [jnp.where(flipped, rows - 1 - row, row) for row in range(rows)]
    row = lax.dynamic_index_in_dim(density, order[0], 0, keepdims=False)
    arriving = paired(row, "lat", [(0, 1)])
    even = [1 - lax.axis_index(axis) % 2 for axis in ("lon", "lev")]
    info = jnp.stack([*order, *even]).astype(jnp.int32)
    rest = None
    for step in range(STEPS):
        start, final = step == 0, step == STEPS - 1
        field = density if start else rest
        first = None if start else row
        sent = edges(info, first, field)
        ghosts = exchanged(sent)
        done = rest_step(info, first, field, crowding, ghosts, final)
        rest = done[0]
        ended = done[2] if final else None
        row_done = row_step(info, row, arriving, field, crowding, ghosts, start, ended)
        row = row_done[0]
        if not final:
            arriving = paired(row, "lat", [(0, 1)])
    halves = halves_of_lines(done[1], n)
    row_halves = halves_of_lines(row_done[1][:, None], n)
    scaled = scale(info, (1, 2, 3), rest, *halves)
    scaled = scale(info, (0,), row, *row_halves, scaled)
    return scaled, row_done[2]


def solution(mesh):
    placed = P(("trial", "lat"), "lon", "lev", None)
    return jax.shard_map(
        steps,
        mesh=mesh,
        in_specs=(placed, placed),
        out_specs=(placed, placed),
        check_vma=False,
    )
```

```python
import functools

import jax
import jax.numpy as jnp
from jax import lax
from jax.experimental import pallas as pl
from jax.experimental.pallas import tpu as pltpu
from jax.sharding import PartitionSpec as P


STEPS = 4
CUTS = ((0, 64, 128),) * 4
MIB = 1 << 20
EVEN_X, EVEN_Z = 4, 5
VMEM = pl.BlockSpec(memory_space=pltpu.VMEM)
SMEM = pl.BlockSpec(memory_space=pltpu.SMEM)
ANY = pl.BlockSpec(memory_space=pl.ANY)


def cost(size, flops, reads):
    return pl.CostEstimate(flops=flops * size, bytes_accessed=4 * reads * size, transcendentals=0)


def cells(a, low_x, high_x, near, far, low_z, high_z, crowding):
    length = a.shape[0]
    z = lax.broadcasted_iota(jnp.int32, a.shape, 0)
    down = jnp.where(z == 0, low_z, pltpu.roll(a, 1, 0))
    up = jnp.where(z == length - 1, high_z, pltpu.roll(a, length - 1, 0))
    spread = low_x + high_x + near + far + down + up - 6.0 * a
    return a + 0.1 * spread + 0.2 * a * (1.0 - a * crowding)


def over_x(n, visit, carry=0):
    carry = visit(0, None, 1, carry)
    carry = lax.fori_loop(1, n - 1, lambda x, c: visit(x, x - 1, x + 1, c), carry)
    return visit(n - 1, n - 2, None, carry)


def line_sums(column, n):
    mean = lax.fori_loop(1, n, lambda x, s: s + column(x), column(0)) / n

    def add(x, s):
        d = column(x) - mean
        return s + d * d

    return mean, lax.fori_loop(0, n, add, jnp.zeros_like(mean))


def sides(info, row, ghosts):
    lon_a, lon_b, lev_a, lev_b = ghosts
    even_x, even_z = info[EVEN_X] == 1, info[EVEN_Z] == 1
    low_x = lambda: jnp.where(even_x, lon_b[row], lon_a[row])
    high_x = lambda: jnp.where(even_x, lon_a[row], lon_b[row])

    def ends_z(x):
        a, b = lev_a[row, pl.ds(x, 1), :], lev_b[row, pl.ds(x, 1), :]
        return jnp.where(even_z, b, a), jnp.where(even_z, a, b)

    return low_x, high_x, ends_z


def edge_kernel(count, mapped, info, *refs):
    first, field, sent = refs[:count], refs[count:-4], refs[-4:]
    lon_a, lon_b, lev_a, lev_b = sent
    rows = [None] * (count > 0)
    if field:
        rows += [info[row] if mapped else row for row in range(4 if mapped else 3)]
    n, length = lev_a.shape[1], lon_a.shape[1]
    at_x, at_z = info[EVEN_X] * (n - 1), info[EVEN_Z] * (length - 1)
    for k, row in enumerate(rows):
        for lon, lev, x_at, z_at in (
            (lon_a, lev_a, at_x, at_z),
            (lon_b, lev_b, n - 1 - at_x, length - 1 - at_z),
        ):
            if row is None:
                begin = 0
                for part in first:
                    depth = part.shape[1]
                    lon[k, begin : begin + depth] = part[x_at]
                    begin += depth
                for x in range(n):
                    low, high = first[0][x, 0:1, :], first[-1][x, depth - 1 : depth, :]
                    lev[k, x : x + 1, :] = jnp.where(z_at == 0, low, high)
            else:
                values = field[0].at[row]
                lon[k] = values[x_at]
                for x in range(n):
                    lev[k, x : x + 1, :] = values[x, pl.ds(z_at, 1), :]


def edges(info, first, field, mapped=False):
    args = [*first, *([] if field is None else [field])]
    n, species = args[0].shape[-3], args[0].shape[-1]
    length = sum(part.shape[1] for part in first) if first else field.shape[2]
    rows = (4 if mapped else 3) * (field is not None) + (len(first) > 0)
    lon = jax.ShapeDtypeStruct((rows, length, species), jnp.float32)
    lev = jax.ShapeDtypeStruct((rows, n, species), jnp.float32)
    return pl.pallas_call(
        functools.partial(edge_kernel, len(first), mapped),
        out_shape=[lon, lon, lev, lev],
        in_specs=[SMEM] + [VMEM] * len(args),
        out_specs=[VMEM] * 4,
        compiler_params=pltpu.CompilerParams(vmem_limit_bytes=16 * MIB),
        cost_estimate=cost(2 * rows * (length + n) * species, 1, 2),
        name="edges",
    )(info, *args)


def row_kernel(spans, mapped, low_open, high_open, final, info, *refs):
    centre, received, field, crowding, lon_a, lon_b, lev_a, lev_b = refs[:8]
    refs = refs[8:]
    below, refs = (None, refs) if low_open else (refs[0], refs[1:])
    above, refs = (None, refs) if high_open else (refs[0], refs[1:])
    n = centre.shape[0]
    begin, end = spans[0][0], spans[-1][1]
    even_x, even_z = info[EVEN_X] == 1, info[EVEN_Z] == 1
    second = info[1] if mapped else 0
    here = info[0]

    def visit(x, before, after, carry):
        a, b = lon_a[0, begin:end], lon_b[0, begin:end]
        low_x = jnp.where(even_x, b, a) if before is None else centre[before]
        high_x = jnp.where(even_x, a, b) if after is None else centre[after]
        a, b = lev_a[0, pl.ds(x, 1), :], lev_b[0, pl.ds(x, 1), :]
        low_z = jnp.where(even_z, b, a) if low_open else below[x, below.shape[1] - 1 :, :]
        high_z = jnp.where(even_z, a, b) if high_open else above[x, 0:1, :]
        near, far = received[x], field[second, x, begin:end]
        value = cells(
            centre[x], low_x, high_x, near, far, low_z, high_z, crowding[here, x, begin:end]
        )
        for (a, b), out in zip(spans, outs):
            out[x] = value[a - begin : b - begin]
        return carry

    outs = refs[: len(spans)]
    over_x(n, visit)
    if final:
        refs[-1][0], refs[-1][1] = line_sums(lambda x: outs[0][x], n)


def row_step(info, p, parts, received, cuts, next_cuts, field, crowding, ghosts, mapped, final):
    n, depth, species = parts[p].shape
    begin, end = cuts[p], cuts[p + 1]
    spans = [(a, b) for a, b in zip(next_cuts[:-1], next_cuts[1:]) if begin <= a and b <= end]
    low_open, high_open = p == 0, p == len(parts) - 1
    out_shape = [jax.ShapeDtypeStruct((n, b - a, species), jnp.float32) for a, b in spans]
    if final:
        out_shape.append(jax.ShapeDtypeStruct((2, depth, species), jnp.float32))
    args = [parts[p], received, field, crowding, *ghosts]
    args += [] if low_open else [parts[p - 1]]
    args += [] if high_open else [parts[p + 1]]
    return pl.pallas_call(
        functools.partial(row_kernel, spans, mapped, low_open, high_open, final),
        in_specs=[SMEM] + [VMEM] * len(args),
        out_specs=[VMEM] * len(out_shape),
        out_shape=out_shape,
        compiler_params=pltpu.CompilerParams(vmem_limit_bytes=20 * MIB),
        cost_estimate=cost(parts[p].size, 20, 5),
    )(info, *args)


def rest_kernel(count, mapped, rows, ghost_from, final, info, *refs):
    first, refs = refs[:count], refs[count:]
    field, crowding, lon_a, lon_b, lev_a, lev_b = refs[:6]
    refs = refs[6:]
    if final:
        out, sums, ended, sem = refs[-4:]
    else:
        out = refs[-1]
    n, length = field.shape[1], field.shape[2]
    copies = []
    for k, row in enumerate(rows):
        at = info[row + 1] if mapped else row
        beyond = info[row + 2] if mapped and row < 2 else row + 1
        crowd_at = info[row + 1]
        low, high, ends_z = sides(info, row - ghost_from, (lon_a, lon_b, lev_a, lev_b))

        def visit(x, before, after, carry):
            low_x = low() if before is None else field[at, before]
            high_x = high() if after is None else field[at, after]
            if mapped:
                near = field[info[row], x]
            elif row:
                near = field[row - 1, x]
            else:
                near = jnp.concatenate([part[x] for part in first], axis=0)
            far = 0.0 if row == 2 else field[beyond, x]
            low_z, high_z = ends_z(x)
            out[k, x] = cells(
                field[at, x], low_x, high_x, near, far, low_z, high_z, crowding[crowd_at, x]
            )
            return carry

        over_x(n, visit)
        if final:
            copies.append(pltpu.make_async_copy(out.at[k], ended.at[info[row + 1]], sem.at[k]))
            copies[-1].start()
            there = slice(k * length, (k + 1) * length)
            sums[0, there], sums[1, there] = line_sums(lambda x: out[k, x], n)
    for copy in copies:
        copy.wait()


def rest_step(info, first, field, crowding, ghosts, mapped, rows=(0, 1, 2), ghost_from=-1, final=False, ended=None):
    _, n, length, species = field.shape
    count = len(rows)
    out_shape = [jax.ShapeDtypeStruct((count, n, length, species), jnp.float32)]
    out_specs, scratch, more = [VMEM], [], {}
    args = [*first, field, crowding, *ghosts]
    in_specs = [SMEM] + [VMEM] * len(args)
    if final:
        out_shape += [
            jax.ShapeDtypeStruct((2, count * length, species), jnp.float32),
            jax.ShapeDtypeStruct((4, n, length, species), jnp.float32),
        ]
        out_specs += [VMEM, ANY]
        scratch = [pltpu.SemaphoreType.DMA((count,))]
        if ended is not None:
            args.append(ended)
            in_specs.append(ANY)
            more = {"input_output_aliases": {len(args): 2}}
    return pl.pallas_call(
        functools.partial(rest_kernel, len(first), mapped, rows, ghost_from, final),
        out_shape=out_shape,
        in_specs=in_specs,
        out_specs=out_specs,
        scratch_shapes=scratch,
        compiler_params=pltpu.CompilerParams(vmem_limit_bytes=24 * MIB),
        cost_estimate=cost(count * n * length * species, 20, 4),
        name="rest",
        **more,
    )(info, *args)


def merged(a, b, n):
    d = a[0] - b[0]
    return jnp.stack([0.5 * (a[0] + b[0]), a[1] + b[1] + (0.5 * n) * d * d])


def line_factors(a, b, n):
    d = a[0] - b[0]
    variance = (a[1] + b[1] + (0.5 * n) * d * d) / (2 * n)
    return 0.5 * (a[0] + b[0]), lax.rsqrt(variance + 0.0001)


def scale_kernel(rows, begins, info, *refs):
    count = len(begins)
    fields, (one, two) = refs[:count], refs[count : count + 2]
    scaled, ended, buffers, sem = refs[-3 - count], refs[-2 - count], refs[-1 - count : -1], refs[-1]
    n = buffers[0].shape[-3]
    jobs = []
    for field, buffer, begin in zip(fields, buffers, begins):
        if begin is None:
            jobs += [(field.at[k], buffer.at[k], info[row], 0, False) for k, row in enumerate(rows)]
        else:
            jobs.append((field, buffer, info[0], begin, True))
    copies, line = [], 0

    def copy(source, target, row, begin):
        there = target.at[row, :, begin : begin + source.shape[1]]
        copies.append(pltpu.make_async_copy(source, there, sem.at[len(copies)]))
        copies[-1].start()

    for field, _, row, begin, place in jobs:
        if place:
            copy(field, ended, row, begin)
    for field, buffer, row, begin, _ in jobs:
        lines = slice(line, line + field.shape[1])
        line += field.shape[1]
        mean, factor = line_factors(*([s[0, lines], s[1, lines]] for s in (one, two)), 2 * n)

        def visit(x, carry):
            buffer[x] = (field[x] - mean) * factor
            return carry

        lax.fori_loop(0, n, visit, 0)
        copy(buffer, scaled, row, begin)
    for c in copies:
        c.wait()


def scale(info, fields, rows, begins, one, two, ended, scaled=None):
    extra = [ended] if scaled is None else [ended, scaled]
    at = 3 + len(fields)
    size = sum(field.size for field in fields)
    return pl.pallas_call(
        functools.partial(scale_kernel, rows, begins),
        out_shape=[jax.ShapeDtypeStruct(ended.shape, jnp.float32)] * 2,
        in_specs=[SMEM] + [VMEM] * (len(fields) + 2) + [ANY] * len(extra),
        out_specs=[ANY, ANY],
        scratch_shapes=[
            *(pltpu.VMEM(field.shape, jnp.float32) for field in fields),
            pltpu.SemaphoreType.DMA((8,)),
        ],
        input_output_aliases={at: 1} if scaled is None else {at: 1, at + 1: 0},
        compiler_params=pltpu.CompilerParams(vmem_limit_bytes=16 * MIB),
        cost_estimate=cost(size, 3, 2),
        name="scale",
    )(info, *fields, one, two, *extra)


def paired(array, axis, pairs):
    return lax.ppermute(array, axis, [*pairs, *((b, a) for a, b in pairs)])


def exchanged(sent):
    lon_a, lon_b, lev_a, lev_b = sent
    return (
        paired(lon_a, "lon", [(0, 1), (2, 3)]),
        paired(lon_b, "lon", [(1, 2)]),
        paired(lev_a, "lev", [(0, 1), (2, 3), (4, 5), (6, 7)]),
        paired(lev_b, "lev", [(1, 2), (3, 4), (5, 6)]),
    )


def halves_of_lines(sums, n):
    half = merged(sums, paired(sums, "lon", [(0, 1), (2, 3)]), n)
    return half, paired(half, "lon", [(0, 2), (1, 3)])


def steps(density, crowding):
    rows, n, _, species = density.shape
    flipped = lax.axis_index("lat") == 0
    order = [jnp.where(flipped, rows - 1 - row, row) for row in range(rows)]

    def swapped(parts):
        return [paired(part, "lat", [(0, 1)]) for part in parts]

    parts = [
        lax.dynamic_slice(density, (order[0], 0, a, 0), (1, n, b - a, species))[0]
        for a, b in zip(CUTS[0][:-1], CUTS[0][1:])
    ]
    arriving = swapped(parts)
    even = [1 - lax.axis_index(axis) % 2 for axis in ("lon", "lev")]
    info = jnp.stack([*order, *even]).astype(jnp.int32)
    rest = None
    for step in range(STEPS):
        start, final = step == 0, step == STEPS - 1
        cuts = CUTS[step]
        next_cuts = cuts if final else CUTS[step + 1]
        field = density if start else rest
        first = [] if start else parts
        sent = edges(info, first, None if final else field, start)
        ghosts = exchanged(sent)
        if final:
            sent = edges(info, [], rest)
            ghosts_rest = exchanged(sent)
            deep, deep_sums, ended = rest_step(
                info, [], rest, crowding, ghosts_rest, False, (1, 2), 0, True
            )
            beside, beside_sums, ended = rest_step(
                info, first, rest, crowding, ghosts_rest, False, (0,), 0, True, ended
            )
        else:
            (rest,) = rest_step(info, first, field, crowding, ghosts, start)
        new = []
        for p in range(len(parts)):
            new += row_step(
                info, p, parts, arriving[p], cuts, next_cuts, field, crowding, ghosts, start, final
            )
        if not final:
            parts = new
            arriving = swapped(parts)
    first, first_sums, last, last_sums = new
    lines = halves_of_lines(deep_sums, n)
    scaled, ended = scale(info, [deep], (2, 3), [None], *lines, ended)
    lines = halves_of_lines(jnp.concatenate([beside_sums, first_sums], axis=1), n)
    scaled, ended = scale(info, [beside, first], (1,), [None, 0], *lines, ended, scaled)
    lines = halves_of_lines(last_sums, n)
    scaled, ended = scale(info, [last], (), [cuts[1]], *lines, ended, scaled)
    return scaled, ended


def solution(mesh):
    placed = P(("trial", "lat"), "lon", "lev", None)
    return jax.shard_map(
        steps,
        mesh=mesh,
        in_specs=(placed, placed),
        out_specs=(placed, placed),
        check_vma=False,
    )
```

```python
import functools

import jax
import jax.numpy as jnp
from jax import lax
from jax.experimental import pallas as pl
from jax.experimental.pallas import tpu as pltpu
from jax.sharding import PartitionSpec as P


STEPS = 4
CUTS = (0, 64, 128)
MIB = 1 << 20
EVEN_X, EVEN_Z = 4, 5
VMEM = pl.BlockSpec(memory_space=pltpu.VMEM)
SMEM = pl.BlockSpec(memory_space=pltpu.SMEM)
ANY = pl.BlockSpec(memory_space=pl.ANY)


def cost(size, flops, reads):
    return pl.CostEstimate(flops=flops * size, bytes_accessed=4 * reads * size, transcendentals=0)


def cells(a, low_x, high_x, near, far, low_z, high_z, crowding):
    length = a.shape[0]
    z = lax.broadcasted_iota(jnp.int32, a.shape, 0)
    down = jnp.where(z == 0, low_z, pltpu.roll(a, 1, 0))
    up = jnp.where(z == length - 1, high_z, pltpu.roll(a, length - 1, 0))
    spread = low_x + high_x + near + far + down + up - 6.0 * a
    return a + 0.1 * spread + 0.2 * a * (1.0 - a * crowding)


def over_x(n, visit, carry=0):
    carry = visit(0, None, 1, carry)
    carry = lax.fori_loop(1, n - 1, lambda x, c: visit(x, x - 1, x + 1, c), carry)
    return visit(n - 1, n - 2, None, carry)


def line_sums(column, n):
    mean = lax.fori_loop(1, n, lambda x, s: s + column(x), column(0)) / n

    def add(x, s):
        d = column(x) - mean
        return s + d * d

    return mean, lax.fori_loop(0, n, add, jnp.zeros_like(mean))


def sides(info, row, ghosts):
    lon_a, lon_b, lev_a, lev_b = ghosts
    even_x, even_z = info[EVEN_X] == 1, info[EVEN_Z] == 1
    low_x = lambda: jnp.where(even_x, lon_b[row], lon_a[row])
    high_x = lambda: jnp.where(even_x, lon_a[row], lon_b[row])

    def ends_z(x):
        a, b = lev_a[row, pl.ds(x, 1), :], lev_b[row, pl.ds(x, 1), :]
        return jnp.where(even_z, b, a), jnp.where(even_z, a, b)

    return low_x, high_x, ends_z


def edge_kernel(count, mapped, info, *refs):
    first, field, sent = refs[:count], refs[count:-4], refs[-4:]
    lon_a, lon_b, lev_a, lev_b = sent
    rows = [None] * (count > 0)
    if field:
        rows += [info[row] if mapped else row for row in range(4 if mapped else 3)]
    n, length = lev_a.shape[1], lon_a.shape[1]
    at_x, at_z = info[EVEN_X] * (n - 1), info[EVEN_Z] * (length - 1)
    for k, row in enumerate(rows):
        for lon, lev, x_at, z_at in (
            (lon_a, lev_a, at_x, at_z),
            (lon_b, lev_b, n - 1 - at_x, length - 1 - at_z),
        ):
            if row is None:
                begin = 0
                for part in first:
                    depth = part.shape[1]
                    lon[k, begin : begin + depth] = part[x_at]
                    begin += depth
                for x in range(n):
                    low, high = first[0][x, 0:1, :], first[-1][x, depth - 1 : depth, :]
                    lev[k, x : x + 1, :] = jnp.where(z_at == 0, low, high)
            else:
                values = field[0].at[row]
                lon[k] = values[x_at]
                for x in range(n):
                    lev[k, x : x + 1, :] = values[x, pl.ds(z_at, 1), :]


def edges(info, first, field, mapped=False):
    args = [*first, *([] if field is None else [field])]
    n, species = args[0].shape[-3], args[0].shape[-1]
    length = sum(part.shape[1] for part in first) if first else field.shape[2]
    rows = (4 if mapped else 3) * (field is not None) + (len(first) > 0)
    lon = jax.ShapeDtypeStruct((rows, length, species), jnp.float32)
    lev = jax.ShapeDtypeStruct((rows, n, species), jnp.float32)
    return pl.pallas_call(
        functools.partial(edge_kernel, len(first), mapped),
        out_shape=[lon, lon, lev, lev],
        in_specs=[SMEM] + [VMEM] * len(args),
        out_specs=[VMEM] * 4,
        compiler_params=pltpu.CompilerParams(vmem_limit_bytes=16 * MIB),
        cost_estimate=cost(2 * rows * (length + n) * species, 1, 2),
        name="edges",
    )(info, *args)


def row_kernel(begin, mapped, low_open, high_open, final, info, *refs):
    centre, received, field, crowding, lon_a, lon_b, lev_a, lev_b = refs[:8]
    refs = refs[8:]
    below, refs = (None, refs) if low_open else (refs[0], refs[1:])
    above, refs = (None, refs) if high_open else (refs[0], refs[1:])
    n, depth = centre.shape[0], centre.shape[1]
    end = begin + depth
    even_x, even_z = info[EVEN_X] == 1, info[EVEN_Z] == 1
    second = info[1] if mapped else 0
    here = info[0]

    def visit(x, before, after, carry):
        a, b = lon_a[0, begin:end], lon_b[0, begin:end]
        low_x = jnp.where(even_x, b, a) if before is None else centre[before]
        high_x = jnp.where(even_x, a, b) if after is None else centre[after]
        a, b = lev_a[0, pl.ds(x, 1), :], lev_b[0, pl.ds(x, 1), :]
        low_z = jnp.where(even_z, b, a) if low_open else below[x, below.shape[1] - 1 :, :]
        high_z = jnp.where(even_z, a, b) if high_open else above[x, 0:1, :]
        near, far = received[x], field[second, x, begin:end]
        out[x] = cells(
            centre[x], low_x, high_x, near, far, low_z, high_z, crowding[here, x, begin:end]
        )
        return carry

    out = refs[0]
    over_x(n, visit)
    if final:
        refs[1][0], refs[1][1] = line_sums(lambda x: out[x], n)


def row_step(info, p, parts, received, cuts, field, crowding, ghosts, mapped, final):
    n, depth, species = parts[p].shape
    low_open, high_open = p == 0, p == len(parts) - 1
    out_shape = [jax.ShapeDtypeStruct((n, depth, species), jnp.float32)]
    if final:
        out_shape.append(jax.ShapeDtypeStruct((2, depth, species), jnp.float32))
    args = [parts[p], received, field, crowding, *ghosts]
    args += [] if low_open else [parts[p - 1]]
    args += [] if high_open else [parts[p + 1]]
    return pl.pallas_call(
        functools.partial(row_kernel, cuts[p], mapped, low_open, high_open, final),
        in_specs=[SMEM] + [VMEM] * len(args),
        out_specs=[VMEM] * len(out_shape),
        out_shape=out_shape,
        compiler_params=pltpu.CompilerParams(vmem_limit_bytes=20 * MIB),
        cost_estimate=cost(parts[p].size, 20, 5),
    )(info, *args)


def rest_kernel(count, mapped, rows, ghost_from, final, info, *refs):
    first, refs = refs[:count], refs[count:]
    field, crowding, lon_a, lon_b, lev_a, lev_b = refs[:6]
    refs = refs[6:]
    if final:
        out, sums, ended, sem = refs[-4:]
    else:
        out = refs[-1]
    n, length = field.shape[1], field.shape[2]
    copies = []
    for k, row in enumerate(rows):
        at = info[row + 1] if mapped else row
        beyond = info[row + 2] if mapped and row < 2 else row + 1
        crowd_at = info[row + 1]
        low, high, ends_z = sides(info, row - ghost_from, (lon_a, lon_b, lev_a, lev_b))

        def visit(x, before, after, carry):
            low_x = low() if before is None else field[at, before]
            high_x = high() if after is None else field[at, after]
            if mapped:
                near = field[info[row], x]
            elif row:
                near = field[row - 1, x]
            else:
                near = jnp.concatenate([part[x] for part in first], axis=0)
            far = 0.0 if row == 2 else field[beyond, x]
            low_z, high_z = ends_z(x)
            out[k, x] = cells(
                field[at, x], low_x, high_x, near, far, low_z, high_z, crowding[crowd_at, x]
            )
            return carry

        over_x(n, visit)
        if final:
            copies.append(pltpu.make_async_copy(out.at[k], ended.at[info[row + 1]], sem.at[k]))
            copies[-1].start()
            there = slice(k * length, (k + 1) * length)
            sums[0, there], sums[1, there] = line_sums(lambda x: out[k, x], n)
    for copy in copies:
        copy.wait()


def rest_step(info, first, field, crowding, ghosts, mapped, rows=(0, 1, 2), ghost_from=-1, final=False, ended=None):
    _, n, length, species = field.shape
    count = len(rows)
    out_shape = [jax.ShapeDtypeStruct((count, n, length, species), jnp.float32)]
    out_specs, scratch, more = [VMEM], [], {}
    args = [*first, field, crowding, *ghosts]
    in_specs = [SMEM] + [VMEM] * len(args)
    if final:
        out_shape += [
            jax.ShapeDtypeStruct((2, count * length, species), jnp.float32),
            jax.ShapeDtypeStruct((4, n, length, species), jnp.float32),
        ]
        out_specs += [VMEM, ANY]
        scratch = [pltpu.SemaphoreType.DMA((count,))]
        if ended is not None:
            args.append(ended)
            in_specs.append(ANY)
            more = {"input_output_aliases": {len(args): 2}}
    return pl.pallas_call(
        functools.partial(rest_kernel, len(first), mapped, rows, ghost_from, final),
        out_shape=out_shape,
        in_specs=in_specs,
        out_specs=out_specs,
        scratch_shapes=scratch,
        compiler_params=pltpu.CompilerParams(vmem_limit_bytes=24 * MIB),
        cost_estimate=cost(count * n * length * species, 20, 4),
        name="rest",
        **more,
    )(info, *args)


def merged(a, b, n):
    d = a[0] - b[0]
    return jnp.stack([0.5 * (a[0] + b[0]), a[1] + b[1] + (0.5 * n) * d * d])


def line_factors(a, b, n):
    d = a[0] - b[0]
    variance = (a[1] + b[1] + (0.5 * n) * d * d) / (2 * n)
    return 0.5 * (a[0] + b[0]), lax.rsqrt(variance + 0.0001)


def scale_kernel(rows, begins, info, *refs):
    count = len(begins)
    fields, (one, two) = refs[:count], refs[count : count + 2]
    scaled, ended, buffers, sem = refs[-3 - count], refs[-2 - count], refs[-1 - count : -1], refs[-1]
    n = buffers[0].shape[-3]
    jobs = []
    for field, buffer, begin in zip(fields, buffers, begins):
        if begin is None:
            jobs += [(field.at[k], buffer.at[k], info[row], 0, False) for k, row in enumerate(rows)]
        else:
            jobs.append((field, buffer, info[0], begin, True))
    copies, line = [], 0

    def copy(source, target, row, begin):
        there = target.at[row, :, begin : begin + source.shape[1]]
        copies.append(pltpu.make_async_copy(source, there, sem.at[len(copies)]))
        copies[-1].start()

    for field, _, row, begin, place in jobs:
        if place:
            copy(field, ended, row, begin)
    for field, buffer, row, begin, _ in jobs:
        lines = slice(line, line + field.shape[1])
        line += field.shape[1]
        mean, factor = line_factors(*([s[0, lines], s[1, lines]] for s in (one, two)), 2 * n)

        def visit(x, carry):
            buffer[x] = (field[x] - mean) * factor
            return carry

        lax.fori_loop(0, n, visit, 0)
        copy(buffer, scaled, row, begin)
    for c in copies:
        c.wait()


def scale(info, fields, rows, begins, one, two, ended, scaled=None):
    extra = [ended] if scaled is None else [ended, scaled]
    at = 3 + len(fields)
    size = sum(field.size for field in fields)
    return pl.pallas_call(
        functools.partial(scale_kernel, rows, begins),
        out_shape=[jax.ShapeDtypeStruct(ended.shape, jnp.float32)] * 2,
        in_specs=[SMEM] + [VMEM] * (len(fields) + 2) + [ANY] * len(extra),
        out_specs=[ANY, ANY],
        scratch_shapes=[
            *(pltpu.VMEM(field.shape, jnp.float32) for field in fields),
            pltpu.SemaphoreType.DMA((8,)),
        ],
        input_output_aliases={at: 1} if scaled is None else {at: 1, at + 1: 0},
        compiler_params=pltpu.CompilerParams(vmem_limit_bytes=16 * MIB),
        cost_estimate=cost(size, 3, 2),
        name="scale",
    )(info, *fields, one, two, *extra)


def paired(array, axis, pairs):
    return lax.ppermute(array, axis, [*pairs, *((b, a) for a, b in pairs)])


def exchanged(sent):
    lon_a, lon_b, lev_a, lev_b = sent
    return (
        paired(lon_a, "lon", [(0, 1), (2, 3)]),
        paired(lon_b, "lon", [(1, 2)]),
        paired(lev_a, "lev", [(0, 1), (2, 3), (4, 5), (6, 7)]),
        paired(lev_b, "lev", [(1, 2), (3, 4), (5, 6)]),
    )


def halves_of_lines(sums, n):
    half = merged(sums, paired(sums, "lon", [(0, 1), (2, 3)]), n)
    return half, paired(half, "lon", [(0, 2), (1, 3)])


def steps(density, crowding):
    rows, n, _, species = density.shape
    flipped = lax.axis_index("lat") == 0
    order = [jnp.where(flipped, rows - 1 - row, row) for row in range(rows)]

    def swapped(parts):
        return [paired(part, "lat", [(0, 1)]) for part in parts]

    parts = [
        lax.dynamic_slice(density, (order[0], 0, a, 0), (1, n, b - a, species))[0]
        for a, b in zip(CUTS[:-1], CUTS[1:])
    ]
    arriving = swapped(parts)
    even = [1 - lax.axis_index(axis) % 2 for axis in ("lon", "lev")]
    info = jnp.stack([*order, *even]).astype(jnp.int32)
    cuts, last_step = CUTS, STEPS - 1
    sent = edges(info, [], density, True)
    row_ghosts = exchanged(sent)
    (ahead,) = rest_step(info, [], density, crowding, row_ghosts, True)
    sent = edges(info, [], ahead)
    ghosts, ghost_from = exchanged(sent), 0
    field = density
    for step in range(STEPS):
        start, final = step == 0, step == last_step
        if not start:
            field = ahead
        if final:
            sent = edges(info, parts, None)
            row_ghosts = exchanged(sent)
            beside, beside_sums, ended = rest_step(
                info, parts, field, crowding, ghosts, False, (0,), ghost_from, True, ended
            )
        elif not start:
            (ahead,) = rest_step(info, parts, field, crowding, ghosts, False, ghost_from=ghost_from)
            sent = edges(info, parts, ahead)
            row_ghosts = ghosts = exchanged(sent)
            ghost_from = -1
        if step == last_step - 1:
            deep, deep_sums, ended = rest_step(
                info, [], ahead, crowding, ghosts, False, (1, 2), ghost_from, True
            )
        new = []
        for p in range(len(parts)):
            new += row_step(
                info, p, parts, arriving[p], cuts, field, crowding, row_ghosts, start, final
            )
        if not final:
            parts = new
            arriving = swapped(parts)
    first, first_sums, last, last_sums = new
    lines = halves_of_lines(deep_sums, n)
    scaled, ended = scale(info, [deep], (2, 3), [None], *lines, ended)
    lines = halves_of_lines(jnp.concatenate([beside_sums, first_sums], axis=1), n)
    scaled, ended = scale(info, [beside, first], (1,), [None, 0], *lines, ended, scaled)
    lines = halves_of_lines(last_sums, n)
    scaled, ended = scale(info, [last], (), [cuts[1]], *lines, ended, scaled)
    return scaled, ended


def solution(mesh):
    placed = P(("trial", "lat"), "lon", "lev", None)
    return jax.shard_map(
        steps,
        mesh=mesh,
        in_specs=(placed, placed),
        out_specs=(placed, placed),
        check_vma=False,
    )
```

```python
import functools

import jax
import jax.numpy as jnp
from jax import lax
from jax.experimental import pallas as pl
from jax.experimental.pallas import tpu as pltpu
from jax.sharding import PartitionSpec as P


STEPS = 4
CUTS = (0, 64, 128)
MIB = 1 << 20
EVEN_X, EVEN_Z = 4, 5
VMEM = pl.BlockSpec(memory_space=pltpu.VMEM)
SMEM = pl.BlockSpec(memory_space=pltpu.SMEM)
ANY = pl.BlockSpec(memory_space=pl.ANY)


def cost(size, flops, reads):
    return pl.CostEstimate(flops=flops * size, bytes_accessed=4 * reads * size, transcendentals=0)


def cells(a, low_x, high_x, near, far, low_z, high_z, crowding):
    length = a.shape[0]
    z = lax.broadcasted_iota(jnp.int32, a.shape, 0)
    down = jnp.where(z == 0, low_z, pltpu.roll(a, 1, 0))
    up = jnp.where(z == length - 1, high_z, pltpu.roll(a, length - 1, 0))
    spread = low_x + high_x + near + far + down + up - 6.0 * a
    return a + 0.1 * spread + 0.2 * a * (1.0 - a * crowding)


def over_x(n, visit, carry=0):
    carry = visit(0, None, 1, carry)
    carry = lax.fori_loop(1, n - 1, lambda x, c: visit(x, x - 1, x + 1, c), carry)
    return visit(n - 1, n - 2, None, carry)


def line_sums(total, column, n):
    mean = total / n

    def add(x, s):
        d = column(x) - mean
        return s + d * d

    return mean, lax.fori_loop(0, n, add, jnp.zeros_like(mean))


def sides(info, row, ghosts):
    lon_a, lon_b, lev_a, lev_b = ghosts
    even_x, even_z = info[EVEN_X] == 1, info[EVEN_Z] == 1
    low_x = lambda: jnp.where(even_x, lon_b[row], lon_a[row])
    high_x = lambda: jnp.where(even_x, lon_a[row], lon_b[row])

    def ends_z(x):
        a, b = lev_a[row, pl.ds(x, 1), :], lev_b[row, pl.ds(x, 1), :]
        return jnp.where(even_z, b, a), jnp.where(even_z, a, b)

    return low_x, high_x, ends_z


def edge_kernel(count, mapped, info, *refs):
    first, field, sent = refs[:count], refs[count:-4], refs[-4:]
    lon_a, lon_b, lev_a, lev_b = sent
    rows = [None] * (count > 0)
    if field:
        rows += [info[row] if mapped else row for row in range(4 if mapped else 3)]
    n, length = lev_a.shape[1], lon_a.shape[1]
    at_x, at_z = info[EVEN_X] * (n - 1), info[EVEN_Z] * (length - 1)
    for k, row in enumerate(rows):
        for lon, lev, x_at, z_at in (
            (lon_a, lev_a, at_x, at_z),
            (lon_b, lev_b, n - 1 - at_x, length - 1 - at_z),
        ):
            if row is None:
                begin = 0
                for part in first:
                    depth = part.shape[1]
                    lon[k, begin : begin + depth] = part[x_at]
                    begin += depth
                for x in range(n):
                    low, high = first[0][x, 0:1, :], first[-1][x, depth - 1 : depth, :]
                    lev[k, x : x + 1, :] = jnp.where(z_at == 0, low, high)
            else:
                values = field[0].at[row]
                lon[k] = values[x_at]
                for x in range(n):
                    lev[k, x : x + 1, :] = values[x, pl.ds(z_at, 1), :]


def edges(info, first, field, mapped=False):
    args = [*first, *([] if field is None else [field])]
    n, species = args[0].shape[-3], args[0].shape[-1]
    length = sum(part.shape[1] for part in first) if first else field.shape[2]
    rows = (4 if mapped else 3) * (field is not None) + (len(first) > 0)
    lon = jax.ShapeDtypeStruct((rows, length, species), jnp.float32)
    lev = jax.ShapeDtypeStruct((rows, n, species), jnp.float32)
    return pl.pallas_call(
        functools.partial(edge_kernel, len(first), mapped),
        out_shape=[lon, lon, lev, lev],
        in_specs=[SMEM] + [VMEM] * len(args),
        out_specs=[VMEM] * 4,
        compiler_params=pltpu.CompilerParams(vmem_limit_bytes=16 * MIB),
        cost_estimate=cost(2 * rows * (length + n) * species, 1, 2),
        name="edges",
    )(info, *args)


def row_kernel(begin, mapped, low_open, high_open, final, info, *refs):
    centre, received, field, crowding, lon_a, lon_b, lev_a, lev_b = refs[:8]
    refs = refs[8:]
    below, refs = (None, refs) if low_open else (refs[0], refs[1:])
    above, refs = (None, refs) if high_open else (refs[0], refs[1:])
    n, depth = centre.shape[0], centre.shape[1]
    end = begin + depth
    even_x, even_z = info[EVEN_X] == 1, info[EVEN_Z] == 1
    second = info[1] if mapped else 0
    here = info[0]

    def visit(x, before, after, carry):
        a, b = lon_a[0, begin:end], lon_b[0, begin:end]
        low_x = jnp.where(even_x, b, a) if before is None else centre[before]
        high_x = jnp.where(even_x, a, b) if after is None else centre[after]
        a, b = lev_a[0, pl.ds(x, 1), :], lev_b[0, pl.ds(x, 1), :]
        low_z = jnp.where(even_z, b, a) if low_open else below[x, below.shape[1] - 1 :, :]
        high_z = jnp.where(even_z, a, b) if high_open else above[x, 0:1, :]
        near, far = received[x], field[second, x, begin:end]
        value = cells(
            centre[x], low_x, high_x, near, far, low_z, high_z, crowding[here, x, begin:end]
        )
        out[x] = value
        return carry + value if final else carry

    out = refs[0]
    total = over_x(n, visit, jnp.zeros(centre.shape[1:], jnp.float32) if final else 0)
    if final:
        refs[1][0], refs[1][1] = line_sums(total, lambda x: out[x], n)


def row_step(info, p, parts, received, cuts, field, crowding, ghosts, mapped, final):
    n, depth, species = parts[p].shape
    low_open, high_open = p == 0, p == len(parts) - 1
    out_shape = [jax.ShapeDtypeStruct((n, depth, species), jnp.float32)]
    if final:
        out_shape.append(jax.ShapeDtypeStruct((2, depth, species), jnp.float32))
    args = [parts[p], received, field, crowding, *ghosts]
    args += [] if low_open else [parts[p - 1]]
    args += [] if high_open else [parts[p + 1]]
    return pl.pallas_call(
        functools.partial(row_kernel, cuts[p], mapped, low_open, high_open, final),
        in_specs=[SMEM] + [VMEM] * len(args),
        out_specs=[VMEM] * len(out_shape),
        out_shape=out_shape,
        compiler_params=pltpu.CompilerParams(vmem_limit_bytes=20 * MIB),
        cost_estimate=cost(parts[p].size, 20, 5),
    )(info, *args)


def rest_kernel(count, mapped, rows, ghost_from, final, place, info, *refs):
    first, refs = refs[:count], refs[count:]
    field, crowding, lon_a, lon_b, lev_a, lev_b = refs[:6]
    refs = refs[6:]
    out, refs = refs[0], refs[1:]
    sums, refs = (refs[0], refs[1:]) if final else (None, refs)
    n, length = field.shape[1], field.shape[2]
    copies = []
    for k, row in enumerate(rows):
        at = info[row + 1] if mapped else row
        beyond = info[row + 2] if mapped and row < 2 else row + 1
        crowd_at = info[row + 1]
        low, high, ends_z = sides(info, row - ghost_from, (lon_a, lon_b, lev_a, lev_b))

        def visit(x, before, after, carry):
            low_x = low() if before is None else field[at, before]
            high_x = high() if after is None else field[at, after]
            if mapped:
                near = field[info[row], x]
            elif row:
                near = field[row - 1, x]
            else:
                near = jnp.concatenate([part[x] for part in first], axis=0)
            far = 0.0 if row == 2 else field[beyond, x]
            low_z, high_z = ends_z(x)
            value = cells(
                field[at, x], low_x, high_x, near, far, low_z, high_z, crowding[crowd_at, x]
            )
            out[k, x] = value
            return carry + value if final else carry

        total = over_x(n, visit, jnp.zeros(field.shape[2:], jnp.float32) if final else 0)
        if place:
            ended, sem = refs
            copies.append(pltpu.make_async_copy(out.at[k], ended.at[info[row + 1]], sem.at[k]))
            copies[-1].start()
        if final:
            there = slice(k * length, (k + 1) * length)
            sums[0, there], sums[1, there] = line_sums(total, lambda x: out[k, x], n)
    for copy in copies:
        copy.wait()


def rest_step(info, first, field, crowding, ghosts, mapped, rows=(0, 1, 2), ghost_from=-1, final=False, place=False):
    _, n, length, species = field.shape
    count = len(rows)
    out_shape = [jax.ShapeDtypeStruct((count, n, length, species), jnp.float32)]
    out_specs, scratch = [VMEM], []
    args = [*first, field, crowding, *ghosts]
    if final:
        out_shape.append(jax.ShapeDtypeStruct((2, count * length, species), jnp.float32))
        out_specs.append(VMEM)
    if place:
        out_shape.append(jax.ShapeDtypeStruct((4, n, length, species), jnp.float32))
        out_specs.append(ANY)
        scratch = [pltpu.SemaphoreType.DMA((count,))]
    return pl.pallas_call(
        functools.partial(rest_kernel, len(first), mapped, rows, ghost_from, final, place),
        out_shape=out_shape,
        in_specs=[SMEM] + [VMEM] * len(args),
        out_specs=out_specs,
        scratch_shapes=scratch,
        compiler_params=pltpu.CompilerParams(vmem_limit_bytes=24 * MIB),
        cost_estimate=cost(count * n * length * species, 20, 4),
        name="rest",
    )(info, *args)


def merged(a, b, n):
    d = a[0] - b[0]
    return jnp.stack([0.5 * (a[0] + b[0]), a[1] + b[1] + (0.5 * n) * d * d])


def line_factors(a, b, n):
    d = a[0] - b[0]
    variance = (a[1] + b[1] + (0.5 * n) * d * d) / (2 * n)
    return 0.5 * (a[0] + b[0]), lax.rsqrt(variance + 0.0001)


def scale_kernel(rows, begins, places, info, *refs):
    count = len(begins)
    fields, (one, two), refs = refs[:count], refs[count : count + 2], refs[count + 2 :]
    placed, refs = refs[: len(places)], refs[len(places) :]
    scaled, ended, buffers, sem = refs[-3 - count], refs[-2 - count], refs[-1 - count : -1], refs[-1]
    n = buffers[0].shape[-3]
    jobs = []
    for field, buffer, begin in zip(fields, buffers, begins):
        if begin is None:
            jobs += [(field.at[k], buffer.at[k], info[row], 0) for k, row in enumerate(rows)]
        else:
            jobs.append((field, buffer, info[0], begin))
    copies, line = [], 0

    def copy(source, target, row, begin):
        there = target.at[row, :, begin : begin + source.shape[1]]
        copies.append(pltpu.make_async_copy(source, there, sem.at[len(copies)]))
        copies[-1].start()

    for source, (row, begin) in zip(placed, places):
        copy(source if row == 0 else source.at[0], ended, info[row], begin)
    for field, buffer, row, begin in jobs:
        lines = slice(line, line + field.shape[1])
        line += field.shape[1]
        mean, factor = line_factors(*([s[0, lines], s[1, lines]] for s in (one, two)), 2 * n)

        def visit(x, carry):
            buffer[x] = (field[x] - mean) * factor
            return carry

        lax.fori_loop(0, n, visit, 0)
        copy(buffer, scaled, row, begin)
    for c in copies:
        c.wait()


def scale(info, fields, rows, begins, one, two, placed, places, ended, scaled=None):
    extra = [ended] if scaled is None else [ended, scaled]
    at = 3 + len(fields) + len(placed)
    size = sum(field.size for field in fields)
    return pl.pallas_call(
        functools.partial(scale_kernel, rows, begins, places),
        out_shape=[jax.ShapeDtypeStruct(ended.shape, jnp.float32)] * 2,
        in_specs=[SMEM] + [VMEM] * (len(fields) + 2 + len(placed)) + [ANY] * len(extra),
        out_specs=[ANY, ANY],
        scratch_shapes=[
            *(pltpu.VMEM(field.shape, jnp.float32) for field in fields),
            pltpu.SemaphoreType.DMA((8,)),
        ],
        input_output_aliases={at: 1} if scaled is None else {at: 1, at + 1: 0},
        compiler_params=pltpu.CompilerParams(vmem_limit_bytes=16 * MIB),
        cost_estimate=cost(size, 3, 2),
        name="scale",
    )(info, *fields, one, two, *placed, *extra)


def paired(array, axis, pairs):
    return lax.ppermute(array, axis, [*pairs, *((b, a) for a, b in pairs)])


def exchanged(sent):
    lon_a, lon_b, lev_a, lev_b = sent
    return (
        paired(lon_a, "lon", [(0, 1), (2, 3)]),
        paired(lon_b, "lon", [(1, 2)]),
        paired(lev_a, "lev", [(0, 1), (2, 3), (4, 5), (6, 7)]),
        paired(lev_b, "lev", [(1, 2), (3, 4), (5, 6)]),
    )


def halves_of_lines(sums, n):
    half = merged(sums, paired(sums, "lon", [(0, 1), (2, 3)]), n)
    return half, paired(half, "lon", [(0, 2), (1, 3)])


def steps(density, crowding):
    rows, n, _, species = density.shape
    flipped = lax.axis_index("lat") == 0
    order = [jnp.where(flipped, rows - 1 - row, row) for row in range(rows)]

    def swapped(parts):
        return [paired(part, "lat", [(0, 1)]) for part in parts]

    parts = [
        lax.dynamic_slice(density, (order[0], 0, a, 0), (1, n, b - a, species))[0]
        for a, b in zip(CUTS[:-1], CUTS[1:])
    ]
    arriving = swapped(parts)
    even = [1 - lax.axis_index(axis) % 2 for axis in ("lon", "lev")]
    info = jnp.stack([*order, *even]).astype(jnp.int32)
    cuts, last_step = CUTS, STEPS - 1
    sent = edges(info, [], density, True)
    row_ghosts = exchanged(sent)
    (ahead,) = rest_step(info, [], density, crowding, row_ghosts, True)
    sent = edges(info, [], ahead)
    ghosts, ghost_from = exchanged(sent), 0
    field = density
    for step in range(STEPS):
        start, final = step == 0, step == last_step
        if not start:
            field = ahead
        if final:
            sent = edges(info, parts, None)
            row_ghosts = exchanged(sent)
            beside, beside_sums = rest_step(
                info, parts, field, crowding, ghosts, False, (0,), ghost_from, True
            )
        elif not start:
            (ahead,) = rest_step(info, parts, field, crowding, ghosts, False, ghost_from=ghost_from)
            sent = edges(info, parts, ahead)
            row_ghosts = ghosts = exchanged(sent)
            ghost_from = -1
        if step == last_step - 1:
            deep, deep_sums, ended = rest_step(
                info, [], ahead, crowding, ghosts, False, (1, 2), ghost_from, True, True
            )
        new = []
        for p in range(len(parts)):
            new += row_step(
                info, p, parts, arriving[p], cuts, field, crowding, row_ghosts, start, final
            )
        if not final:
            parts = new
            arriving = swapped(parts)
    first, first_sums, last, last_sums = new
    lines = halves_of_lines(deep_sums, n)
    scaled, ended = scale(info, [deep], (2, 3), [None], *lines, [], [], ended)
    lines = halves_of_lines(jnp.concatenate([beside_sums, first_sums], axis=1), n)
    scaled, ended = scale(
        info,
        [beside, first],
        (1,),
        [None, 0],
        *lines,
        [beside, first, last],
        [(1, 0), (0, 0), (0, cuts[1])],
        ended,
        scaled,
    )
    lines = halves_of_lines(last_sums, n)
    scaled, ended = scale(info, [last], (), [cuts[1]], *lines, [], [], ended, scaled)
    return scaled, ended


def solution(mesh):
    placed = P(("trial", "lat"), "lon", "lev", None)
    return jax.shard_map(
        steps,
        mesh=mesh,
        in_specs=(placed, placed),
        out_specs=(placed, placed),
        check_vma=False,
    )
```
